256 devices in a mesh: seq: 32 (over y, x, z_lo), head: 8 (over z_hi, core).
Axes of the slice: x: 4, y: 4, z: 8 (z_hi: 4, z_lo: 2; z = z_hi * 2 + z_lo), core: 2. Of those that a mesh axis runs over, the one named last changes fastest.
Arguments:
- queries: bfloat16 [8192, 4096], P(('seq', 'head')), may hold values from -10 to 10
- keys: bfloat16 [8192, 1024], P(('seq', 'head')), may hold values from -10 to 10
- block_pos: int32 [64], replicated, may hold values from 0 to 63, each once
- query_map: float32 [32, 128, 128], P('head'), may hold values from -4 to 4
- key_map: float32 [8, 128, 128], P('head'), may hold values from -4 to 4
Outputs:
- query_map_gradient: float32 [32, 128, 128], P('head')
- key_map_gradient: float32 [8, 128, 128], P('head')
The draws below stay inside these ranges and needn't reach their ends.
Inputs may be any that keep to these rules, and one draw needn't show every extreme that they name: A permutation: stored block g (token rows g * 128 to (g + 1) * 128 - 1) holds position block block_pos[g]; position blocks below 32 form the first sequence, the others the second.
All inputs are finite; a program needn't handle non-finite values.
Results may differ from the reference program's by a relative error of at most 0.0021.
Values may be sent and summed in bfloat16 or wider, within the bound.
A program may use at most 64 MiB of HBM per device.

```python
import math
import jax
import jax.numpy as jnp
from jax import lax

QUERY_HEAD_COUNT = 32
KEY_HEAD_COUNT = 8
HEAD_SIZE = 128
BLK = 128
TOKEN_TOTAL = 8192
N_SEQ = 32


def field_pair(key):
    base_offset = jax.random.fold_in(key, 7)
    key_feature_field = jnp.clip(jax.random.normal(jax.random.fold_in(base_offset, 1), (TOKEN_TOTAL, KEY_HEAD_COUNT, HEAD_SIZE), jnp.float32), -4.0, 4.0)
    query_feature_field = jnp.clip(jax.random.normal(jax.random.fold_in(base_offset, 2), (TOKEN_TOTAL, KEY_HEAD_COUNT, QUERY_HEAD_COUNT // KEY_HEAD_COUNT, HEAD_SIZE), jnp.float32), -4.0, 4.0)
    return (query_feature_field.reshape(TOKEN_TOTAL, QUERY_HEAD_COUNT * HEAD_SIZE), key_feature_field.reshape(TOKEN_TOTAL, KEY_HEAD_COUNT * HEAD_SIZE))


def feature_map_values(key, head_count):
    values = jnp.clip(jax.random.normal(key, (head_count, HEAD_SIZE, HEAD_SIZE), jnp.float32), -4.0, 4.0) / math.sqrt(HEAD_SIZE)
    return values


def draw_queries(key, part):
    return field_pair(key)[0].astype(jnp.bfloat16)


def draw_keys(key, part):
    return field_pair(key)[1].astype(jnp.bfloat16)


def draw_query_map(key, part):
    return feature_map_values(jax.random.fold_in(key, 11), QUERY_HEAD_COUNT)


def draw_key_map(key, part):
    return feature_map_values(jax.random.fold_in(key, 13), KEY_HEAD_COUNT)


def setup_inputs(seed: int = 0) -> dict:
    key_list = jax.random.split(jax.random.key(seed), 6)
    return {
        "queries": draw_queries(jax.random.fold_in(key_list[5], 71), 0),
        "keys": draw_keys(jax.random.fold_in(key_list[5], 71), 0),
        "block_pos": jax.random.permutation(key_list[2], 2 * N_SEQ).astype(jnp.int32),
        "query_map": draw_query_map(jax.random.fold_in(key_list[5], 71), 0),
        "key_map": draw_key_map(jax.random.fold_in(key_list[5], 71), 0),
    }


HIGHEST = lax.Precision.HIGHEST
NEG_FLOOR = -1e+30

def softmax_pair(logits):
    return jnp.concatenate([jax.nn.softmax(logits, axis=-1), jax.nn.softmax(-logits, axis=-1)], axis=-1)

def feature_grad(feature, upstream):
    half_width = feature.shape[-1] // 2
    positive, negative = (feature[..., :half_width], feature[..., half_width:])
    grad_positive, grad_negative = (upstream[..., :half_width], upstream[..., half_width:])
    first = positive * (grad_positive - lax.optimization_barrier(jnp.sum(grad_positive * positive, axis=-1, keepdims=True)))
    second = negative * (grad_negative - lax.optimization_barrier(jnp.sum(grad_negative * negative, axis=-1, keepdims=True)))
    return first - second

def reference(queries, keys, block_pos, query_map, key_map):
    token_count = queries.shape[0]
    group_width = QUERY_HEAD_COUNT // KEY_HEAD_COUNT
    row_index = jnp.arange(token_count, dtype=jnp.int32)
    blocks = block_pos[row_index // BLK]
    seq_ids = blocks // N_SEQ
    places = blocks * BLK + row_index % BLK
    block_count = token_count // BLK
    score_scale = HEAD_SIZE ** (-0.5)

    def single_head(kv_index):
        key_rows = lax.dynamic_slice_in_dim(keys, kv_index * HEAD_SIZE, HEAD_SIZE, 1)
        key_wide = key_rows.astype(jnp.float32)
        phi_key = softmax_pair(jnp.dot(key_wide, key_map[kv_index], precision=HIGHEST))
        phi_key_b = phi_key.astype(jnp.bfloat16)
        query_rows = lax.dynamic_slice_in_dim(queries, kv_index * group_width * HEAD_SIZE, group_width * HEAD_SIZE, 1)
        query_heads = query_rows.reshape(token_count, group_width, HEAD_SIZE).transpose(1, 0, 2)
        query_wide = query_heads.astype(jnp.float32)
        head_maps = lax.dynamic_slice_in_dim(query_map, kv_index * group_width, group_width, 0)
        phi_query = softmax_pair(jnp.einsum('gtd,gde->gte', query_wide, head_maps, precision=HIGHEST))
        phi_query_b = phi_query.astype(jnp.bfloat16)

        def one_block(key_grad, number):
            query_block = lax.dynamic_slice_in_dim(query_heads, number * BLK, BLK, 1).reshape(group_width * BLK, HEAD_SIZE)
            phi_block = lax.dynamic_slice_in_dim(phi_query_b, number * BLK, BLK, 1).reshape(group_width * BLK, 2 * HEAD_SIZE)
            block_seq = jnp.tile(lax.dynamic_slice_in_dim(seq_ids, number * BLK, BLK), group_width)
            block_place = jnp.tile(lax.dynamic_slice_in_dim(places, number * BLK, BLK), group_width)
            visible = (seq_ids[None, :] == block_seq[:, None]) & (places[None, :] <= block_place[:, None])
            scores = jnp.dot(query_block, key_rows.T, preferred_element_type=jnp.float32) * score_scale
            masked = jnp.where(visible, scores, NEG_FLOOR)
            highest = lax.optimization_barrier(jnp.max(masked, axis=-1, keepdims=True))
            exponent = jnp.where(visible, jnp.exp(masked - highest), 0.0)
            teacher_prob = exponent / lax.optimization_barrier(jnp.sum(exponent, axis=-1, keepdims=True))
            linear = jnp.dot(phi_block, phi_key_b.T, preferred_element_type=jnp.float32)
            linear_sum = lax.optimization_barrier(jnp.sum(jnp.where(visible, linear, 0.0), axis=-1, keepdims=True))
            weights = (jnp.where(visible, 1.0 / linear_sum - teacher_prob / linear, 0.0) / token_count).astype(jnp.bfloat16)
            query_grad = jnp.dot(weights, phi_key_b, preferred_element_type=jnp.float32)
            key_grad = key_grad + jnp.dot(weights.T, phi_block, preferred_element_type=jnp.float32)
            return (key_grad, query_grad)
        key_grad, query_grads = lax.scan(one_block, jnp.zeros((token_count, 2 * HEAD_SIZE), jnp.float32), jnp.arange(block_count, dtype=jnp.int32))
        query_grad = query_grads.reshape(block_count, group_width, BLK, 2 * HEAD_SIZE).transpose(1, 0, 2, 3).reshape(group_width, token_count, 2 * HEAD_SIZE)
        query_weight_grad = jnp.einsum('gtd,gte->gde', query_wide, feature_grad(phi_query, query_grad), precision=HIGHEST)
        key_weight_grad = jnp.dot(key_wide.T, feature_grad(phi_key, key_grad), precision=HIGHEST)
        return (query_weight_grad, key_weight_grad)
    query_map_gradient, key_map_gradient = lax.map(single_head, jnp.arange(KEY_HEAD_COUNT, dtype=jnp.int32))
    return (query_map_gradient.reshape(QUERY_HEAD_COUNT, HEAD_SIZE, HEAD_SIZE), key_map_gradient)
```

```python
import functools
import math

import jax
import jax.numpy as jnp
from jax import lax
from jax.experimental import pallas as pl
from jax.experimental.pallas import tpu as pltpu
from jax.sharding import PartitionSpec as P

MESH = pl.DeviceIdType.MESH
BF16 = jnp.bfloat16
F32 = jnp.float32
NEG = -1e30
TOKENS = 8192
SCALE = 128 ** (-0.5)
EXP2_SCALE = SCALE * math.log2(math.e)


def place():
    s, h = lax.axis_index("seq"), lax.axis_index("head")
    y, x, zl = s // 8, (s // 2) % 4, s % 2
    zh, c = h // 2, h % 2
    return y, x, zh, zl, c


def device(y, x, z, c):
    return {"seq": (y * 4 + x) * 2 + z % 2, "head": (z // 2) * 2 + c}


class Copies:
    def __init__(self, send, recv):
        self.send, self.recv, self.count = send, recv, 0
        self.started = []

    def start(self, src, dst, to):
        copy = pltpu.make_async_remote_copy(
            src_ref=src, dst_ref=dst, send_sem=self.send.at[self.count],
            recv_sem=self.recv.at[self.count], device_id=to, device_id_type=MESH)
        self.count += 1
        copy.start()
        self.started.append(copy)
        return copy

    def finish(self):
        for copy in self.started:
            copy.wait_send()


EXCHANGE_COPIES = 112


def exchange_kernel(q_ref, k_ref, wq_ref, wk_ref, qall, kall, wqr, wkr, landed, send, recv):
    y, x, zh, zl, c = place()
    z = zh * 2 + zl
    b, z2 = zl * 2 + zh // 2, zh % 2
    quarter = z2 * 2 + c
    net = Copies(send, recv)

    def cols(block, width):
        return pl.ds(pl.multiple_of(block * width, width), width)

    kall[y, x, b, z2, c] = k_ref[:, cols(z, 128)]
    landed[quarter, b] = q_ref[pl.ds(pl.multiple_of(c * 16, 16), 16), cols(z, 512)]

    barrier = pltpu.get_barrier_semaphore()
    for dz in range(8):
        for dc in range(2):
            if dz or dc:
                pl.semaphore_signal(barrier, inc=1, device_id=device(y, x, (z + dz) % 8, (c + dc) % 2), device_id_type=MESH)
    for dy in range(4):
        for dx in range(4):
            if dy or dx:
                pl.semaphore_signal(barrier, inc=1, device_id=device((y + dy) % 4, (x + dx) % 4, z, c), device_id_type=MESH)
    pl.semaphore_wait(barrier, 30)

    partner = device(y, x, z, 1 - c)
    k_first = []
    for dz in (4, 3, 5, 2, 6, 1, 7):
        to = (z + dz) % 8
        k_first.append(net.start(k_ref.at[:, cols(to, 128)], kall.at[y, x, b, z2, c], device(y, x, to, c)))
    q_first = []
    for dz in (4, 3, 5, 2, 6, 1, 7, 0):
        for dc in range(2):
            if dz or dc:
                to, core = (z + dz) % 8, (c + dc) % 2
                q_first.append(net.start(
                    q_ref.at[pl.ds(pl.multiple_of(core * 16, 16), 16), cols(to, 512)],
                    landed.at[quarter, b], device(y, x, to, core)))
    maps = [net.start(wq_ref.at[y], wqr, partner), net.start(wk_ref.at[0], wkr, partner)]

    def piece(y0, x0, half):
        return kall.at[y0, x0, pl.ds(2 * half, 2), :, c]

    for copy in k_first:
        copy.wait_recv()
    direct = {}
    for d in (2, 1, 3):
        for half in range(2):
            src = piece(y, x, half)
            direct[half, 0, d] = net.start(src, src, device(y, (x + d) % 4, z, c))
            direct[half, d, 0] = net.start(src, src, device((y + d) % 4, x, z, c))
    shared = []
    for half in range(2):
        src = piece(y, x, half)
        shared.append(net.start(src, src, partner))
    relayed = {}
    for d in (1, 3, 2):
        direct[0, 0, d].wait_recv()
        src = piece(y, (x - d) % 4, 0)
        for e in (2, 1, 3):
            relayed[0, e, d] = net.start(src, src, device((y + e) % 4, x, z, c))
        shared.append(net.start(src, src, partner))
        direct[1, d, 0].wait_recv()
        src = piece((y - d) % 4, x, 1)
        for e in (2, 1, 3):
            relayed[1, d, e] = net.start(src, src, device(y, (x + e) % 4, z, c))
        shared.append(net.start(src, src, partner))
    for d in (1, 3, 2):
        direct[1, 0, d].wait_recv()
        src = piece(y, (x - d) % 4, 1)
        shared.append(net.start(src, src, partner))
        direct[0, d, 0].wait_recv()
        src = piece((y - d) % 4, x, 0)
        shared.append(net.start(src, src, partner))

    for copy in q_first:
        copy.wait_recv()
    q_second = []
    for dy in (2, 1, 3, 0):
        for dx in (2, 1, 3, 0):
            if dy or dx:
                y1, x1 = (y + dy) % 4, (x + dx) % 4
                q_second.append(net.start(
                    landed.at[x1, :, :, cols(y1, 128)], qall.at[y * 4 + x], device(y1, x1, z, c)))
    qall[y * 4 + x] = landed[x, :, :, cols(y, 128)]

    for dx in (1, 3, 2):
        for dy in (1, 3, 2):
            for half in range(2):
                relayed[half, dy, dx].wait_recv()
                src = piece((y - dy) % 4, (x - dx) % 4, half)
                shared.append(net.start(src, src, partner))
    for copy in maps + q_second + shared:
        copy.wait_recv()
    net.finish()


def exchange(queries, keys, query_map, key_map):
    vmem = pl.BlockSpec(memory_space=pltpu.VMEM)
    return pl.pallas_call(
        exchange_kernel,
        out_shape=(
            jax.ShapeDtypeStruct((16, 4, 16, 128), BF16),
            jax.ShapeDtypeStruct((4, 4, 4, 2, 2, 32, 128), BF16),
            jax.ShapeDtypeStruct((128, 128), F32),
            jax.ShapeDtypeStruct((128, 128), F32),
        ),
        in_specs=[vmem] * 4,
        out_specs=(vmem,) * 4,
        scratch_shapes=[
            pltpu.VMEM((4, 4, 16, 512), BF16),
            pltpu.SemaphoreType.DMA((EXCHANGE_COPIES,)),
            pltpu.SemaphoreType.DMA((EXCHANGE_COPIES,)),
        ],
        compiler_params=pltpu.CompilerParams(collective_id=0, has_side_effects=True),
        name="exchange",
    )(queries, keys, query_map, key_map)


def dot_nt(a, b):
    return lax.dot_general(a, b, (((1,), (1,)), ((), ())), preferred_element_type=F32)


def dot_nn(a, b):
    return lax.dot_general(a, b, (((1,), (0,)), ((), ())), preferred_element_type=F32)


def split3(a):
    hi = a.astype(BF16)
    rest = a - hi.astype(F32)
    mid = rest.astype(BF16)
    lo = (rest - mid.astype(F32)).astype(BF16)
    return jnp.concatenate([hi, mid, lo], axis=0)


def add3(p):
    return p[:128] + (p[128:256] + p[256:])


def softmax_pair_t(logits):
    up = jnp.exp(logits - jnp.max(logits, axis=0, keepdims=True))
    down = jnp.exp(jnp.min(logits, axis=0, keepdims=True) - logits)
    up = up * (1.0 / jnp.sum(up, axis=0, keepdims=True))
    down = down * (1.0 / jnp.sum(down, axis=0, keepdims=True))
    return up, down


def feature_grad_t(up, down, grad):
    grad_up, grad_down = grad[:128], grad[128:]
    first = up * (grad_up - jnp.sum(grad_up * up, axis=0, keepdims=True))
    second = down * (grad_down - jnp.sum(grad_down * down, axis=0, keepdims=True))
    return first - second


CH = 512


def compute_kernel(inv, q_ref, k_ref, wq_own, wq_got, wk_own, wk_got, out_q, out_k,
                   wq3, wk3, qs, ks, kf, kb, qf, qtb, qb, t_ref, s_ref, w_ref, gq, acc_q, acc_k):
    y, x, zh, zl, c = place()
    own = zl == c

    @pl.when(own)
    def _():
        wq3[...] = split3(wq_own[y].T)
        wk3[...] = split3(wk_own[0].T)

    @pl.when(jnp.logical_not(own))
    def _():
        wq3[...] = split3(wq_got[...].T)
        wk3[...] = split3(wk_got[...].T)

    acc_q[...] = jnp.zeros_like(acc_q)
    acc_k[...] = jnp.zeros_like(acc_k)
    first_row = (2 * x + c) * 16
    row = lax.broadcasted_iota(jnp.int32, (128, CH), 0)
    last_live = (row // 16) * 128 + row % 16 + first_row
    key = lax.broadcasted_iota(jnp.int32, (128, CH), 1)

    def live(j):
        return key + j * CH <= last_live

    def one_sequence(number, carry):
        def gather(p, inner):
            stored = inv[number * 32 + p]
            qs[pl.ds(pl.multiple_of(p * 16, 16), 16), :] = q_ref[stored]
            ks[pl.ds(pl.multiple_of(p * 128, 128), 128), :] = k_ref[stored]
            return inner

        lax.fori_loop(0, 32, gather, 0)

        def key_features(j, inner):
            at = pl.multiple_of(j * CH, CH)
            up, down = softmax_pair_t(add3(dot_nt(wk3[...], ks[pl.ds(at, CH), :])))
            kf[0:128, pl.ds(at, CH)] = up
            kf[128:256, pl.ds(at, CH)] = down
            kb[0:128, pl.ds(at, CH)] = up.astype(BF16)
            kb[128:256, pl.ds(at, CH)] = down.astype(BF16)
            return inner

        lax.fori_loop(0, 4096 // CH, key_features, 0)
        up, down = softmax_pair_t(add3(dot_nt(wq3[...], qs[...])))
        qf[0:128] = up
        qf[128:256] = down
        qtb[0:128] = up.astype(BF16)
        qtb[128:256] = down.astype(BF16)
        qb[:, 0:128] = up.T.astype(BF16)
        qb[:, 128:256] = down.T.astype(BF16)

        for r in range(4):
            rows = slice(128 * r, 128 * r + 128)
            per = 1024 // CH
            chunks = per * (r + 1)
            q_tile = qs[rows, :]
            phi_tile = qb[rows, :]
            high = jnp.full((128, 128), NEG, F32)
            for j in range(chunks):
                t = dot_nt(q_tile, ks[j * CH:(j + 1) * CH, :])
                if j >= per * r:
                    t = jnp.where(live(j - per * r), t, NEG)
                t_ref[:, j * CH:(j + 1) * CH] = t
                for k in range(CH // 128):
                    high = jnp.maximum(high, t[:, k * 128:(k + 1) * 128])
            high = jnp.max(high, axis=1, keepdims=True)
            den = jnp.zeros((128, 128), F32)
            lin = jnp.zeros((128, 128), F32)
            for j in range(chunks):
                e = jnp.exp2((t_ref[:, j * CH:(j + 1) * CH] - high) * EXP2_SCALE)
                t_ref[:, j * CH:(j + 1) * CH] = e
                s = dot_nn(phi_tile, kb[:, j * CH:(j + 1) * CH])
                s_ref[:, j * CH:(j + 1) * CH] = s
                if j >= per * r:
                    s = jnp.where(live(j - per * r), s, 0.0)
                for k in range(CH // 128):
                    den = den + e[:, k * 128:(k + 1) * 128]
                    lin = lin + s[:, k * 128:(k + 1) * 128]
            den = (1.0 / TOKENS) / jnp.sum(den, axis=1, keepdims=True)
            lin = (1.0 / TOKENS) / jnp.sum(lin, axis=1, keepdims=True)
            for j in range(chunks):
                cut = slice(j * CH, (j + 1) * CH)
                w = lin - (t_ref[:, cut] * den) / s_ref[:, cut]
                if j >= per * r:
                    w = jnp.where(live(j - per * r), w, 0.0)
                w_ref[rows, cut] = w.astype(BF16)
            n = 1024 * (r + 1)
            gq[rows, :] = dot_nt(w_ref[rows, 0:n], kb[:, 0:n])

        for j in range(4096 // CH):
            top = 128 * (j * CH // 1024)
            cut = slice(j * CH, (j + 1) * CH)
            grad = dot_nn(qtb[:, top:512], w_ref[top:512, cut])
            d = feature_grad_t(kf[0:128, cut], kf[128:256, cut], grad)
            acc_k[...] += add3(dot_nn(split3(d), ks[cut, :]))
        d = feature_grad_t(qf[0:128], qf[128:256], gq[...].T)
        acc_q[...] += add3(dot_nn(split3(d), qs[...]))
        return carry

    lax.fori_loop(0, 2, one_sequence, 0)
    out_q[...] = acc_q[...].T
    out_k[...] = acc_k[...].T


def compute(inv, q, k, wq_own, wq_got, wk_own, wk_got):
    vmem = pl.BlockSpec(memory_space=pltpu.VMEM)
    return pl.pallas_call(
        compute_kernel,
        out_shape=(jax.ShapeDtypeStruct((128, 128), F32),) * 2,
        in_specs=[pl.BlockSpec(memory_space=pltpu.SMEM)] + [vmem] * 6,
        out_specs=(vmem,) * 2,
        scratch_shapes=[
            pltpu.VMEM((384, 128), BF16),
            pltpu.VMEM((384, 128), BF16),
            pltpu.VMEM((512, 128), BF16),
            pltpu.VMEM((4096, 128), BF16),
            pltpu.VMEM((256, 4096), F32),
            pltpu.VMEM((256, 4096), BF16),
            pltpu.VMEM((256, 512), F32),
            pltpu.VMEM((256, 512), BF16),
            pltpu.VMEM((512, 256), BF16),
            pltpu.VMEM((128, 4096), F32),
            pltpu.VMEM((128, 4096), F32),
            pltpu.VMEM((512, 4096), BF16),
            pltpu.VMEM((512, 256), F32),
            pltpu.VMEM((128, 128), F32),
            pltpu.VMEM((128, 128), F32),
        ],
        name="compute",
    )(inv, q, k, wq_own, wq_got, wk_own, wk_got)


REDUCE_COPIES = 128


def reduce_kernel(pq, pk, out_q, out_k, got_q, got_k, sum_q, sum_k, send_q, recv_q, send_k, recv_k, bsend_q, brecv_q, bsend_k, brecv_k):
    y, x, zh, zl, c = place()
    z = zh * 2 + zl
    owner = c == zl
    other = zh * 2 + (1 - zl)

    barrier = pltpu.get_barrier_semaphore()
    for dy in range(4):
        for dx in range(4):
            for plane in range(2):
                for dc in range(2):
                    if dy or dx or plane or dc:
                        pl.semaphore_signal(
                            barrier, inc=1,
                            device_id=device((y + dy) % 4, (x + dx) % 4, zh * 2 + (zl + plane) % 2, (c + dc) % 2),
                            device_id_type=MESH)

    mine = 2 * x + c
    got_q[mine] = pq[pl.ds(pl.multiple_of(mine * 16, 16), 16), :]
    slot = y * 4 + x

    @pl.when(owner)
    def _():
        got_k[2 * slot + c] = pk[pl.ds(pl.multiple_of(slot * 8, 8), 8), :]

    pl.semaphore_wait(barrier, 63)

    def send_to(src, dst, sems, rsems, at, to):
        return pltpu.make_async_remote_copy(
            src_ref=src, dst_ref=dst, send_sem=sems.at[at], recv_sem=rsems.at[at], device_id=to, device_id_type=MESH)

    def k_copy(dy, dx, dc):
        y1, x1 = (y + dy) % 4, (x + dx) % 4
        at = ((dy * 4) + dx) * 2 + dc
        return send_to(pk.at[pl.ds(pl.multiple_of((y1 * 4 + x1) * 8, 8), 8), :], got_k.at[2 * slot + c],
                       send_k, recv_k, at, device(y1, x1, z, zl))

    def q_copy(dx, dc):
        x1, c1 = (x + dx) % 4, (c + dc) % 2
        return send_to(pq.at[pl.ds(pl.multiple_of((2 * x1 + c1) * 16, 16), 16), :], got_q.at[mine],
                       send_q, recv_q, dx * 2 + dc, device(y, x1, z, c1))

    far = [(dy, dx) for dy in (2, 1, 3, 0) for dx in (2, 1, 3, 0)]
    for dy, dx in far:
        if dy or dx:
            @pl.when(owner)
            def _(dy=dy, dx=dx):
                k_copy(dy, dx, 0).start()

            @pl.when(jnp.logical_not(owner))
            def _(dy=dy, dx=dx):
                k_copy(dy, dx, 1).start()
        else:
            @pl.when(jnp.logical_not(owner))
            def _():
                k_copy(0, 0, 1).start()
    for dx in (2, 1, 3, 0):
        for dc in range(2):
            if dx or dc:
                q_copy(dx, dc).start()

    for dx in (0, 1, 3, 2):
        for dc in range(2):
            if dx or dc:
                q_copy(dx, dc).wait_recv()
    total = got_q[0]
    for i in range(1, 8):
        total = total + got_q[i]
    sum_q[...] = total

    @pl.when(owner)
    def _():
        for dy, dx in far:
            for dc in range(2):
                if dy or dx or dc:
                    k_copy(dy, dx, dc).wait_recv()
        total = got_k[0]
        for i in range(1, 32):
            total = total + got_k[i]
        sum_k[...] = total

    rows_q = pl.ds(pl.multiple_of(mine * 16, 16), 16)
    rows_k = pl.ds(pl.multiple_of(slot * 8, 8), 8)

    def q_out(dy, dx, plane, core):
        to = zh * 2 + (zl + plane) % 2
        at = ((dy * 4 + dx) * 2 + plane) * 2 + core
        return send_to(sum_q, out_q.at[y, rows_q, :], bsend_q, brecv_q, at, device((y + dy) % 4, (x + dx) % 4, to, zl))

    def k_out(dy, dx, plane):
        to = zh * 2 + (zl + plane) % 2
        at = (dy * 4 + dx) * 2 + plane
        return send_to(sum_k, out_k.at[0, rows_k, :], bsend_k, brecv_k, at, device((y + dy) % 4, (x + dx) % 4, to, zl))

    def sends(act):
        for plane in (1, 0):
            for dy, dx in far:
                @pl.when(owner)
                def _(dy=dy, dx=dx, plane=plane):
                    if dy or dx or plane:
                        act(q_out(dy, dx, plane, 0))
                        act(k_out(dy, dx, plane))

                @pl.when(jnp.logical_not(owner))
                def _(dy=dy, dx=dx, plane=plane):
                    act(q_out(dy, dx, plane, 1))

    sends(lambda copy: copy.start())

    @pl.when(owner)
    def _():
        out_q[y, rows_q, :] = sum_q[...]
        out_k[0, rows_k, :] = sum_k[...]
        for dy, dx in far:
            for core in range(2):
                if dy or dx or core:
                    q_out(dy, dx, 0, core).wait_recv()
            if dy or dx:
                k_out(dy, dx, 0).wait_recv()

    @pl.when(jnp.logical_not(owner))
    def _():
        for dy, dx in far:
            for core in range(2):
                q_out(dy, dx, 1, core).wait_recv()
            k_out(dy, dx, 1).wait_recv()

    sends(lambda copy: copy.wait_send())
    for dy, dx in far:
        @pl.when(owner)
        def _(dy=dy, dx=dx):
            if dy or dx:
                k_copy(dy, dx, 0).wait_send()

        @pl.when(jnp.logical_not(owner))
        def _(dy=dy, dx=dx):
            k_copy(dy, dx, 1).wait_send()
    for dx in range(4):
        for dc in range(2):
            if dx or dc:
                q_copy(dx, dc).wait_send()


def reduce(pq, pk):
    vmem = pl.BlockSpec(memory_space=pltpu.VMEM)
    dma = pltpu.SemaphoreType.DMA
    return pl.pallas_call(
        reduce_kernel,
        out_shape=(jax.ShapeDtypeStruct((4, 128, 128), F32), jax.ShapeDtypeStruct((1, 128, 128), F32)),
        in_specs=[vmem] * 2,
        out_specs=(vmem,) * 2,
        scratch_shapes=[
            pltpu.VMEM((8, 16, 128), F32),
            pltpu.VMEM((32, 8, 128), F32),
            pltpu.VMEM((16, 128), F32),
            pltpu.VMEM((8, 128), F32),
            dma((8,)), dma((8,)), dma((32,)), dma((32,)),
            dma((64,)), dma((64,)), dma((32,)), dma((32,)),
        ],
        compiler_params=pltpu.CompilerParams(collective_id=1, has_side_effects=True),
        name="reduce",
    )(pq, pk)


def per_device(queries, keys, block_pos, query_map, key_map):
    order = jnp.arange(64, dtype=jnp.int32)
    inv = jnp.sum(jnp.where(block_pos[None, :] == order[:, None], order[None, :], 0), axis=1, dtype=jnp.int32)
    q, k, wq_got, wk_got = exchange(queries, keys, query_map, key_map)
    pq, pk = compute(inv, q.reshape(64, 16, 128), k.reshape(64, 128, 128), query_map, wq_got, key_map, wk_got)
    return reduce(pq, pk)


def solution(mesh):
    in_specs = (
        P(("seq", "head"), None),
        P(("seq", "head"), None),
        P(),
        P("head", None, None),
        P("head", None, None),
    )
    out_specs = (P("head", None, None), P("head", None, None))
    return jax.shard_map(
        per_device, mesh=mesh, in_specs=in_specs, out_specs=out_specs, check_vma=False
    )
```
